32 devices in a mesh: tm: 2 (over core), stn: 4 (over z), chan: 4 (over y, x).
Axes of the slice: x: 2, y: 2, z: 4, core: 2. Of those that a mesh axis runs over, the one named last changes fastest.
Arguments:
- voltages: bfloat16 [2, 8, 512, 32, 2, 256], P(None, 'chan', 'stn', 'tm'), may hold values from -100 to 100
- fir_taps: float32 [16, 256], replicated, may hold values from -1.5 to 1.5
- station_map: int32 [512], P('stn'), may hold values from 0 to 31, as said below
- beam_index: int32 [512], P('stn'), may hold values from 0 to 15
- weight_table: bfloat16 [2, 16, 8, 8], P(None, None, 'chan'), may hold values from -1.5 to 1.5
Outputs:
- visibilities: float32 [2, 2, 8, 32, 32, 8, 2, 2, 256], P('tm', None, 'chan', 'stn')
The draws below stay inside these ranges and needn't reach their ends.
Inputs may be any that keep to these rules, and one draw needn't show every extreme that they name: `station_map`: each station number names exactly 16 dishes; of the dishes g * 128 up to (g + 1) * 128 - 1, exactly 32 name a station of the block h * 8 up to (h + 1) * 8 - 1, for every g and h.
All inputs are finite; a program needn't handle non-finite values.
Results may differ from the reference program's by a relative error of at most 0.017.
Values may be sent and summed in bfloat16 or wider, within the bound.
A program may use at most 512 MiB of HBM per device.

```python
import jax
import jax.numpy as jnp
from jax import lax

DISHES = 512
STATIONS = 32
DPS = 16
BEAMS = 8
POL = 2
COARSE = 8
FINE = 256
TAPS = 16
NTAB = 16
FRAMES_DEV = 16
FRAMES = 32
N_TM = 2
N_STN = 4


def draw_voltages(key, part):
    noise_key, sample_key, frame_key = jax.random.split(jax.random.fold_in(key, 11), 3)
    shape = (2, COARSE, DISHES, FRAMES, POL, FINE)
    noise_draw = jnp.clip(jax.random.normal(noise_key, shape, jnp.float32), -6.0, 6.0)
    rise_factor = 3.0
    coarse_pos = jnp.arange(COARSE, dtype=jnp.float32) / max(COARSE - 1, 1)
    coarse_amp = jnp.sqrt(rise_factor ** coarse_pos)
    sample_amp = 10.0 ** (0.5 * jax.random.uniform(sample_key, (FINE,), jnp.float32))
    frame_amp = 3.0 ** (0.5 * jax.random.uniform(frame_key, (FRAMES,), jnp.float32))
    scaled = noise_draw * coarse_amp[None, :, None, None, None, None] * frame_amp[None, None, None, :, None, None] * sample_amp
    return scaled.astype(jnp.bfloat16)


def draw_station_map(key, part):
    group_dishes = DISHES // N_STN
    share = group_dishes // N_STN
    owned = STATIONS // N_STN
    first_key, second_key = jax.random.split(jax.random.fold_in(key, 23), 2)
    base = jnp.arange(group_dishes, dtype=jnp.int32)
    ranks = jax.vmap(lambda sub_key: jax.random.permutation(sub_key, base))(jax.random.split(first_key, N_STN))
    placing = jax.vmap(lambda sub_key: jax.random.permutation(sub_key, base))(jax.random.split(second_key, N_STN))
    owner = ranks // share
    group_ids = jnp.arange(N_STN, dtype=jnp.int32)[:, None]
    column = group_ids * share + ranks % share
    position = placing[owner, column]
    station = owner * owned + position // (DISHES // STATIONS)
    return station.reshape(DISHES).astype(jnp.int32)


def place_ends(values, stream_key, least, largest):
    dims = values.shape
    index_at = [jax.random.randint(jax.random.fold_in(stream_key, axis), (), 0, dims[axis]) for axis in range(len(dims))]
    values = values.at[tuple(index_at)].set(least)
    longest = dims.index(max(dims))
    index_at[longest] = (index_at[longest] + 1) % dims[longest]
    return values.at[tuple(index_at)].set(largest)


def level_of(key, shape, cuts, smallest, largest):
    def one(dim, blocks):
        heights = jax.random.uniform(jax.random.fold_in(jax.random.fold_in(key, 6), dim), (blocks,), jnp.float32, smallest / len(cuts), largest / len(cuts))
        return jnp.repeat(jnp.exp(heights), shape[dim] // blocks).reshape((-1,) + (1,) * (len(shape) - dim - 1))

    level = one(*cuts[0])
    for cut in cuts[1:]:
        level = level * one(*cut)
    return level


def bell_draw(rng, shape, deviation, most, pieces=(), kind=jnp.bfloat16):
    level = level_of(rng, shape, pieces, -0.22, 0.18) if pieces else 1.0
    array = jax.random.normal(rng, shape, jnp.float32) * deviation * level
    return jnp.minimum(jnp.maximum(array, -most), most).astype(kind)


def setup_inputs(seed: int = 0) -> dict:
    seeds = jax.random.split(jax.random.key(seed), 6)
    voltages = draw_voltages(jax.random.fold_in(seeds[5], 71), 0)
    fir_taps = bell_draw(seeds[1], (TAPS, FINE), TAPS ** -0.5, 1.5, (), jnp.float32)
    station_map = draw_station_map(jax.random.fold_in(seeds[5], 71), 0)
    beam_index = place_ends(jax.random.randint(seeds[3], (DISHES,), 0, NTAB), jax.random.fold_in(seeds[3], 1), 0, NTAB - 1).astype(jnp.int32)
    weight_table = bell_draw(seeds[4], (2, NTAB, COARSE, BEAMS), DPS ** -0.5, 1.5, ((2, 4),))
    return {"voltages": voltages, "fir_taps": fir_taps, "station_map": station_map, "beam_index": beam_index, "weight_table": weight_table}


epsilon = 1e-06

def dft_tables(length):
    bin_index = jnp.arange(length, dtype=jnp.int32)
    phase_step = bin_index[:, None] * bin_index[None, :] % length
    angles = phase_step.astype(jnp.float32) * (2.0 * jnp.pi / length)
    return (jnp.cos(angles).astype(jnp.bfloat16), jnp.sin(angles).astype(jnp.bfloat16))

def correlate(normed_slice):
    values = normed_slice.astype(jnp.float32)
    real_part = values[:, 0]
    imag_part = values[:, 1]

    def product(left_beams, right_beams):
        return jnp.einsum('sbfpk,tbfqk->stbpqk', left_beams, right_beams)
    vis_re = product(real_part, real_part) + product(imag_part, imag_part)
    vis_im = product(imag_part, real_part) - product(real_part, imag_part)
    return jnp.stack([vis_re, vis_im]) / FRAMES_DEV

def reference(voltages, fir_taps, station_map, beam_index, weight_table):
    cosine, sine_table = dft_tables(FINE)
    history = TAPS - 1
    group_size = DISHES // N_STN
    station_hot = (station_map[:, None] == jnp.arange(STATIONS, dtype=jnp.int32)[None, :]).astype(jnp.float32)
    table_hot = (beam_index[:, None] == jnp.arange(NTAB, dtype=jnp.int32)[None, :]).astype(jnp.float32)

    def channel_beams(inputs):
        samples, table_slice = inputs
        padded = jnp.pad(samples, ((0, 0), (0, 0), (history, 0), (0, 0), (0, 0)))
        filtered = jnp.zeros(samples.shape, jnp.float32)
        for tap_index in range(TAPS):
            offset = history - tap_index
            filtered = filtered + fir_taps[tap_index] * padded[:, :, offset:offset + FRAMES].astype(jnp.float32)
        filtered = filtered.astype(jnp.bfloat16)
        real_part = filtered[0].reshape(-1, FINE)
        imag_part = filtered[1].reshape(-1, FINE)
        spec_re = jnp.dot(real_part, cosine, preferred_element_type=jnp.float32) + jnp.dot(imag_part, sine_table, preferred_element_type=jnp.float32)
        spec_im = jnp.dot(imag_part, cosine, preferred_element_type=jnp.float32) - jnp.dot(real_part, sine_table, preferred_element_type=jnp.float32)
        spectra_low = jnp.stack([spec_re, spec_im]).reshape(samples.shape).astype(jnp.bfloat16)
        spectra = lax.optimization_barrier(spectra_low).astype(jnp.float32)
        weights = jnp.einsum('dt,otb->odb', table_hot, table_slice.astype(jnp.float32))
        weight_re = weights[0]
        weight_im = weights[1]
        mixing = jnp.stack([jnp.stack([weight_re, -weight_im]), jnp.stack([weight_im, weight_re])])
        steering = station_hot[None, None, :, :, None] * mixing[:, :, :, None, :]
        summed = jnp.zeros((STATIONS, 2, BEAMS, FRAMES, POL, FINE), jnp.float32)
        for dish_group in range(N_STN):
            low_dish = dish_group * group_size
            partial_value = jnp.einsum('oidsb,idfpk->sobfpk', steering[:, :, low_dish:low_dish + group_size], spectra[:, low_dish:low_dish + group_size])
            rounded = lax.optimization_barrier(partial_value.astype(jnp.bfloat16))
            summed = summed + rounded.astype(jnp.float32)
        return summed.astype(jnp.bfloat16)
    formed = lax.map(channel_beams, (jnp.moveaxis(voltages, 1, 0), jnp.moveaxis(weight_table, 2, 0)))
    outputs = []
    for time_block in range(N_TM):
        first_frame = time_block * FRAMES_DEV
        values = formed[:, :, :, :, first_frame:first_frame + FRAMES_DEV].astype(jnp.float32)
        power_sum = lax.optimization_barrier(jnp.sum(values * values, axis=(0, 2, 4, 6)))
        inverse_rms = lax.rsqrt(power_sum / (COARSE * FRAMES_DEV * FINE) + epsilon)
        normed = (values * inverse_rms[None, :, None, :, None, :, None]).astype(jnp.bfloat16)
        visibility = lax.map(correlate, normed)
        outputs.append(jnp.moveaxis(visibility, 0, 1))
    return jnp.stack(outputs)
```

```python
import functools

import jax
import jax.numpy as jnp
from jax import lax
from jax.experimental import pallas as pl
from jax.experimental.pallas import tpu as pltpu
from jax.sharding import PartitionSpec as P

STATIONS = 32
COARSE = 8
LANES = 128
VMEM_LIMIT = 60 * 1024 * 1024

epsilon = 1e-06


def shifted(value, axis, steps):
    count = lax.axis_size(axis)
    first, last = (max(0, -steps), min(count, count - steps))
    return lax.ppermute(value, axis, [(source, source + steps) for source in range(first, last)])


def dft_table(length):
    bin_index = jnp.arange(length, dtype=jnp.int32)
    phase_step = bin_index[:, None] * bin_index[None, :] % length
    angles = phase_step.astype(jnp.float32) * (2.0 * jnp.pi / length)
    cosine = jnp.cos(angles).astype(jnp.bfloat16)
    sine = jnp.sin(angles).astype(jnp.bfloat16)
    top = jnp.concatenate([cosine, -sine], axis=1)
    return jnp.concatenate([top, jnp.concatenate([sine, cosine], axis=1)], axis=0)


def spectra_kernel(n_dest, x_ref, taps_ref, dft_ref, perm_ref, out_ref, fil_ref):
    taps = taps_ref.shape[0]
    frames = out_ref.shape[2]
    dishes, fine = x_ref.shape[3], x_ref.shape[4]
    share = dishes // n_dest
    rows = min(32, dishes)
    group = 2

    def step(i, carry):
        for j in range(group):
            frame = i * group + j
            for o in range(2):
                for low in range(0, dishes, rows):
                    total = jnp.zeros((rows, fine), jnp.float32)
                    for tap in range(taps):
                        sample = x_ref[0, frame + (taps - 1 - tap), o, low : low + rows, :]
                        total = total + taps_ref[tap : tap + 1, :] * sample.astype(jnp.float32)
                    fil_ref[
                        j * dishes + low : j * dishes + low + rows, o * fine : (o + 1) * fine
                    ] = total.astype(jnp.bfloat16)
        spec = jnp.dot(fil_ref[...], dft_ref[...], preferred_element_type=jnp.float32)
        spec = spec.astype(jnp.bfloat16)
        for j in range(group):
            moved = jnp.dot(
                perm_ref[...],
                spec[j * dishes : (j + 1) * dishes],
                preferred_element_type=jnp.float32,
            )
            for dest in range(n_dest):
                for o in range(2):
                    out_ref[dest, 0, i * group + j, o] = moved[
                        dest * share : (dest + 1) * share, o * fine : (o + 1) * fine
                    ].astype(jnp.bfloat16)
        return carry

    lax.fori_loop(0, frames // group, step, 0)


def spectra_of(extended, fir_taps, table, perm, n_dest, frames):
    polars, total_frames, _, dishes, fine = extended.shape
    share = dishes // n_dest
    flops = 2 * polars * frames * dishes * (2 * fine) * (2 * fine + dishes)
    return pl.pallas_call(
        functools.partial(spectra_kernel, n_dest),
        grid=(polars,),
        in_specs=[
            pl.BlockSpec((1, total_frames, 2, dishes, fine), lambda p: (p, 0, 0, 0, 0)),
            pl.BlockSpec(fir_taps.shape, lambda p: (0, 0)),
            pl.BlockSpec(table.shape, lambda p: (0, 0)),
            pl.BlockSpec(perm.shape, lambda p: (0, 0)),
        ],
        out_specs=pl.BlockSpec(
            (n_dest, 1, frames, 2, share, fine), lambda p: (0, p, 0, 0, 0, 0)
        ),
        out_shape=jax.ShapeDtypeStruct((n_dest, polars, frames, 2, share, fine), jnp.bfloat16),
        scratch_shapes=[pltpu.VMEM((2 * dishes, 2 * fine), jnp.bfloat16)],
        compiler_params=pltpu.CompilerParams(vmem_limit_bytes=VMEM_LIMIT),
        cost_estimate=pl.CostEstimate(
            flops=flops * 4, bytes_accessed=extended.size * 4, transcendentals=0
        ),
        name="spectra",
    )(extended, fir_taps, table, perm)


def beams_kernel(x_ref, steer_ref, out_ref, power_ref):
    frames, fine = out_ref.shape[1], out_ref.shape[3]
    power_ref[...] = jnp.zeros_like(power_ref)

    def step(frame, carry):
        terms = x_ref[:, 0, frame]
        if terms.shape[2] % 16:
            terms = terms.astype(jnp.float32).reshape(-1, fine).astype(jnp.bfloat16)
        else:
            terms = terms.reshape(-1, fine)
        formed = jnp.dot(steer_ref[...], terms, preferred_element_type=jnp.float32)
        formed = formed.astype(jnp.bfloat16)
        out_ref[0, frame] = formed
        wide = formed.astype(jnp.float32)
        power_ref[0] += wide * wide
        return carry

    lax.fori_loop(0, frames, step, 0)


def beams_of(spectra, steering):
    groups, polars, frames, _, share, fine = spectra.shape
    rows = steering.shape[0]
    return pl.pallas_call(
        beams_kernel,
        grid=(polars,),
        in_specs=[
            pl.BlockSpec((groups, 1, frames, 2, share, fine), lambda p: (0, p, 0, 0, 0, 0)),
            pl.BlockSpec(steering.shape, lambda p: (0, 0)),
        ],
        out_specs=[
            pl.BlockSpec((1, frames, rows, fine), lambda p: (p, 0, 0, 0)),
            pl.BlockSpec((1, rows, fine), lambda p: (p, 0, 0)),
        ],
        out_shape=[
            jax.ShapeDtypeStruct((polars, frames, rows, fine), jnp.bfloat16),
            jax.ShapeDtypeStruct((polars, rows, fine), jnp.float32),
        ],
        compiler_params=pltpu.CompilerParams(vmem_limit_bytes=VMEM_LIMIT),
        cost_estimate=pl.CostEstimate(
            flops=2 * rows * steering.shape[1] * polars * frames * fine,
            bytes_accessed=spectra.size * 4,
            transcendentals=0,
        ),
        name="beams",
    )(spectra, steering)


def correlate_kernel(beams, left_ref, right_ref, lscale_ref, rscale_ref, *rest):
    out_ref, left, right = rest[-3:]
    polars, frames, rows, fine = left_ref.shape
    own = rows // (2 * beams)
    halves = fine // LANES
    first = pl.program_id(0) == 0

    def widen(source, target):
        def step(i, carry):
            for p in range(polars):
                target[p, i] = source(p, i).astype(jnp.float32)
            return carry

        lax.fori_loop(0, frames, step, 0)

    @pl.when(first)
    def _():
        widen(lambda p, i: left_ref[p, i], left)

    widen(lambda p, i: right_ref[0, p, i], right)

    def pair(index, carry):
        s = index // own
        t = index % own
        srow = pl.multiple_of(s * (2 * beams), 2 * beams)
        trow = pl.multiple_of(t * (2 * beams), 2 * beams)
        for half in range(halves):
            lanes = pl.ds(half * LANES, LANES)
            re = {}
            im = {}
            for f in range(frames):
                lre = [left[p, f, pl.ds(srow, beams), lanes] for p in range(polars)]
                lim = [left[p, f, pl.ds(srow + beams, beams), lanes] for p in range(polars)]
                rre = [right[q, f, pl.ds(trow, beams), lanes] for q in range(polars)]
                rim = [right[q, f, pl.ds(trow + beams, beams), lanes] for q in range(polars)]
                for p in range(polars):
                    for q in range(polars):
                        a = lre[p] * rre[q] + lim[p] * rim[q]
                        b = lim[p] * rre[q] - lre[p] * rim[q]
                        re[p, q] = a if f == 0 else re[p, q] + a
                        im[p, q] = b if f == 0 else im[p, q] + b
            for p in range(polars):
                for q in range(polars):
                    scale = lscale_ref[p, s] * rscale_ref[0, q, t]
                    row = (p * halves + half) * polars + q
                    where = pl.ds(row, beams, stride=polars * polars * halves)
                    out_ref[0, 0, s, t, where, :] = re[p, q] * scale
                    out_ref[1, 0, s, t, where, :] = im[p, q] * scale
        return carry

    lax.fori_loop(0, own * own, pair, 0)


def correlate(index, coarse_dev, beams, left, right, lscale, rscale, previous):
    groups, polars, frames, rows, fine = right.shape
    own = rows // (2 * beams)
    out_rows = beams * polars * polars * (fine // LANES)
    shape = (2, coarse_dev, own, groups * own, out_rows, LANES)
    in_specs = [
        pl.BlockSpec((polars, frames, rows, fine), lambda g: (0, 0, 0, 0)),
        pl.BlockSpec((1, polars, frames, rows, fine), lambda g: (g, 0, 0, 0, 0)),
        pl.BlockSpec(lscale.shape, lambda g: (0, 0, 0, 0)),
        pl.BlockSpec((1,) + rscale.shape[1:], lambda g: (g, 0, 0, 0, 0)),
    ]
    operands = [left, right, lscale, rscale]
    aliases = {}
    if previous is not None:
        in_specs.append(pl.BlockSpec(memory_space=pl.ANY))
        operands.append(previous)
        aliases = {4: 0}
    size = 2 * own * groups * own * out_rows * LANES
    return pl.pallas_call(
        functools.partial(correlate_kernel, beams),
        grid=(groups,),
        in_specs=in_specs,
        out_specs=pl.BlockSpec(
            (2, 1, own, own, out_rows, LANES), lambda g: (0, index, 0, g, 0, 0)
        ),
        out_shape=jax.ShapeDtypeStruct(shape, jnp.float32),
        scratch_shapes=[
            pltpu.VMEM((polars, frames, rows, fine), jnp.float32),
            pltpu.VMEM((polars, frames, rows, fine), jnp.float32),
        ],
        input_output_aliases=aliases,
        compiler_params=pltpu.CompilerParams(vmem_limit_bytes=VMEM_LIMIT),
        cost_estimate=pl.CostEstimate(
            flops=size * 4 * frames * 100, bytes_accessed=size * 4, transcendentals=0
        ),
        name="correlate",
    )(*operands)


def routes(station_map, beam_index, own_count):
    block = station_map // own_count
    groups, dishes = station_map.shape
    order = jnp.arange(dishes, dtype=jnp.int32)
    same = block[:, :, None] == block[:, None, :]
    before = order[None, None, :] < order[None, :, None]
    rank = jnp.sum((same & before).astype(jnp.int32), axis=2)
    place = block * (dishes // groups) + rank
    hot = place[:, None, :] == order[None, :, None]
    station = jnp.sum(jnp.where(hot, station_map[:, None, :], 0), axis=2)
    row = jnp.sum(jnp.where(hot, beam_index[:, None, :], 0), axis=2)
    return hot, station, row


def per_device(voltages, fir_taps, station_map, beam_index, weight_table):
    components, coarse_dev, dishes_dev, frames_dev, polars, fine = voltages.shape
    history = fir_taps.shape[0] - 1
    table_rows, beams = weight_table.shape[1], weight_table.shape[3]
    groups = lax.axis_size("stn")
    own_count = STATIONS // groups
    share = dishes_dev // groups
    me = lax.axis_index("stn")
    earlier = shifted(voltages[:, :, :, frames_dev - history :], "tm", 1)
    table = dft_table(fine)
    both = lax.all_gather(jnp.stack([station_map, beam_index]), "stn")
    hot, station, row = routes(both[:, 0], both[:, 1], own_count)
    perm = lax.dynamic_index_in_dim(hot, me, 0, keepdims=False).astype(jnp.bfloat16)
    station = lax.dynamic_slice_in_dim(station, me * share, share, 1)
    row = lax.dynamic_slice_in_dim(row, me * share, share, 1)
    station_hot = (
        station[:, :, None] - me * own_count == jnp.arange(own_count, dtype=jnp.int32)
    ).astype(jnp.float32)
    table_hot = (row[:, :, None] == jnp.arange(table_rows, dtype=jnp.int32)).astype(jnp.bfloat16)
    weights = jnp.einsum(
        "gdt,otcb->ocgdb", table_hot, weight_table, preferred_element_type=jnp.float32
    )
    mixing = jnp.stack(
        [jnp.stack([weights[0], -weights[1]]), jnp.stack([weights[1], weights[0]])]
    )
    steering = jnp.einsum("gds,oicgdb->csobgid", station_hot, mixing).astype(jnp.bfloat16)
    steering = steering.reshape(coarse_dev, own_count * 2 * beams, groups * 2 * share)

    formed = []
    gathered = []
    power = 0.0
    spectra = []
    for c in range(coarse_dev):
        extended = jnp.concatenate([earlier[:, c], voltages[:, c]], axis=2)
        extended = jnp.transpose(extended, (3, 2, 0, 1, 4))
        terms = spectra_of(extended, fir_taps, table, perm, groups, frames_dev)
        spectra.append(lax.all_to_all(terms, "stn", 0, 0))
    for c in range(coarse_dev):
        values, squares = beams_of(spectra[c], steering[c])
        formed.append(values)
        gathered.append(lax.all_gather(values, "stn"))
        power = power + jnp.sum(squares.reshape(polars, own_count, 2, beams, fine), axis=(2, 4))
    power = lax.psum(power, "chan")
    inverse_rms = lax.rsqrt(power / (COARSE * frames_dev * fine) + epsilon)
    every = lax.all_gather(inverse_rms, "stn")
    lscale = jnp.broadcast_to(
        inverse_rms[..., None] / frames_dev, inverse_rms.shape + (LANES,)
    )
    rscale = jnp.broadcast_to(every[..., None], every.shape + (LANES,))
    result = None
    for c in range(coarse_dev):
        result = correlate(
            c, coarse_dev, beams, formed[c], gathered[c], lscale, rscale, result
        )
    halves = fine // LANES
    result = result.reshape(
        2, coarse_dev, own_count, STATIONS, beams, polars, halves, polars, LANES
    )
    result = jnp.swapaxes(result, 6, 7)
    return result.reshape(
        1, 2, coarse_dev, own_count, STATIONS, beams, polars, polars, fine
    )


def solution(mesh):
    in_specs = (
        P(None, "chan", "stn", "tm", None, None),
        P(),
        P("stn"),
        P("stn"),
        P(None, None, "chan", None),
    )
    out_specs = P("tm", None, "chan", "stn", None, None, None, None, None)
    return jax.shard_map(
        per_device, mesh=mesh, in_specs=in_specs, out_specs=out_specs, check_vma=False
    )
```
